32 devices in a mesh: grp: 4 (over y, x), brick: 8 (over z, core).
Axes of the slice: x: 2, y: 2, z: 4, core: 2. Of those that a mesh axis runs over, the one named last changes fastest.
Arguments:
- coeffs: bfloat16 [8, 4096, 1024], P(None, 'brick'), may hold values from -6 to 6
- tensor: bfloat16 [32, 1024, 1024], P('grp', 'brick'), may hold values from -0.005859375 to 0.005859375
- pairs: int32 [2, 2], replicated, may hold values from 0 to 7
- lateral: int32 [4096], P('brick'), may hold values from 0 to 511
- thermal: float32 [8], replicated, may hold values from 0.5 to 1
Outputs:
- updated: float32 [32, 8, 4096], P(None, None, 'brick')
The draws below stay inside these ranges and needn't reach their ends.
Inputs may be any that keep to these rules, and one draw needn't show every extreme that they name: `pairs`: row p names the species that receives the collision term and the species it collides with. A cell's lateral partner, as an index within the same block of 512 cells.
All inputs are finite; a program needn't handle non-finite values.
Results may differ from the reference program's by a relative error of at most 0.0003.
Values may be sent and summed in bfloat16 or wider, within the bound.
A program may use at most 128 MiB of HBM per device.

```python
import math
import jax
import jax.numpy as jnp
from jax import lax

M = 1024
MODES = 32
SPECIES = 8
PAIRS = 2
PLANE = 128
C_DEV = 512
CELLS = 4096


def set_ends(result, stream_key, least, high):
    dims = result.shape
    spot = [jax.random.randint(jax.random.fold_in(stream_key, axis), (), 0, dims[axis]) for axis in range(len(dims))]
    result = result.at[tuple(spot)].set(least)
    longest = dims.index(max(dims))
    spot[longest] = (spot[longest] + 1) % dims[longest]
    return result.at[tuple(spot)].set(high)


def block_levels(rng, shape, shards, least, largest):
    def one(position, blocks):
        draws = jax.random.uniform(jax.random.fold_in(jax.random.fold_in(rng, 6), position), (blocks,), jnp.float32, least / len(shards), largest / len(shards))
        return jnp.repeat(jnp.exp(draws), shape[position] // blocks).reshape((-1,) + (1,) * (len(shape) - position - 1))

    level = one(*shards[0])
    for cut in shards[1:]:
        level = level * one(*cut)
    return level


def bell_draw(own_key, dims, scale, reach, pieces=(), kind=jnp.bfloat16):
    entries = scale * jax.random.normal(own_key, dims, jnp.float32)
    if pieces:
        entries = entries * block_levels(own_key, dims, pieces, -0.22, 0.18)
    return jnp.clip(entries, -reach, reach).astype(kind)


def setup_inputs(seed: int = 0) -> dict:
    arg_keys = jax.random.split(jax.random.key(seed), 6)
    coeffs = bell_draw(arg_keys[0], (SPECIES, CELLS, M), 1.0, 6.0, ((1, 8),))
    tensor = bell_draw(arg_keys[1], (MODES, M, M), (M * M) ** -0.5, 0.005859375, ((0, 4), (1, 8)))
    pairs = set_ends(jax.random.randint(arg_keys[2], (PAIRS, 2), 0, SPECIES), jax.random.fold_in(arg_keys[2], 1), 0, SPECIES - 1).astype(jnp.int32)
    lateral = set_ends(jax.random.randint(arg_keys[3], (CELLS,), 0, C_DEV), jax.random.fold_in(arg_keys[3], 1), 0, C_DEV - 1).astype(jnp.int32)
    thermal = jnp.clip(jnp.exp(jax.random.uniform(arg_keys[4], (SPECIES,), jnp.float32, math.log(0.5), math.log(1.0))), 0.5, 1.0)
    return {"coeffs": coeffs, "tensor": tensor, "pairs": pairs, "lateral": lateral, "thermal": thermal}


collision_update = 0.5
courant = 0.08
max_speed = 11.0
mixing = 0.2

def advance(extended, first_mode, thermal, partner):
    mode_count = extended.shape[0] - 2
    thermo = thermal[None, :, None, None]
    orders = (first_mode + jnp.arange(mode_count, dtype=jnp.int32)).astype(jnp.float32)[:, None, None, None]
    speed = thermo * (jnp.sqrt(orders) * extended[:mode_count] + jnp.sqrt(orders + 1.0) * extended[2:])
    middle = extended[1:mode_count + 1]
    face = 0.5 * (speed[:, :, :-1] + speed[:, :, 1:]) - 0.5 * max_speed * thermo * (middle[:, :, 1:] - middle[:, :, :-1])
    center = middle[:, :, 1:-1]
    shape_flat = (mode_count, center.shape[1], center.shape[2] * center.shape[3])
    center = center.reshape(shape_flat)
    divergence = (face[:, :, 1:] - face[:, :, :-1]).reshape(shape_flat)
    beside = jnp.take(center, partner, axis=2)
    return center - courant * divergence + mixing * (beside - center)

def reference(coeffs, tensor, pairs, lateral, thermal):
    species, cells, width = coeffs.shape
    modes = tensor.shape[0]
    pair_count = pairs.shape[0]
    left_side = coeffs[pairs[:, 0]].astype(jnp.float32).reshape(pair_count * cells, width)
    right_side = coeffs[pairs[:, 1]].astype(jnp.float32).reshape(pair_count * cells, width)

    def one_mode(slab):
        inner = jnp.dot(right_side, slab.astype(jnp.float32).T, precision=lax.Precision.HIGHEST)
        return lax.optimization_barrier(jnp.sum(left_side * inner, axis=1))
    collide = lax.map(one_mode, tensor).reshape(modes, pair_count, cells)
    indicator_matrix = (pairs[:, 0][:, None] == jnp.arange(species, dtype=jnp.int32)[None, :]).astype(jnp.float32)
    collision_operator = jnp.einsum('quw,ut->qtw', collide, indicator_matrix, precision=lax.Precision.HIGHEST)
    brick_window = jnp.transpose(coeffs[:, :, :modes], (2, 0, 1))
    species_state = brick_window.astype(jnp.float32) + collision_update * collision_operator
    species_state = jnp.pad(species_state, ((1, 1), (0, 0), (0, 0)))
    layers = cells // PLANE
    species_state = species_state.reshape(modes + 2, species, layers, PLANE)
    extended = jnp.concatenate([species_state[:, :, -1:], species_state, species_state[:, :, :1]], axis=2)
    cell_index = jnp.arange(cells, dtype=jnp.int32)
    partner = (cell_index // C_DEV * C_DEV + lateral).astype(jnp.int32)
    return advance(extended, jnp.int32(0), thermal, partner)
```

```python
import math

import jax
import jax.numpy as jnp
from jax import lax
from jax.experimental import pallas as pl
from jax.experimental.pallas import tpu as pltpu
from jax.sharding import PartitionSpec as P

PLANE = 128

collision_update = 0.5
courant = 0.08
max_speed = 11.0
mixing = 0.2

MESH = pl.DeviceIdType.MESH


def lookup(table, index):
    out = jnp.int32(table[0])
    for i in range(1, len(table)):
        out = jnp.where(index == i, jnp.int32(table[i]), out)
    return out


def fused_kernel(dims, coeffs_ref, tensor_ref, lateral_ref, pairs_ref, thermal_ref, o_ref, *scratch):
    (tbuf, rbuf, lbuf, own_left, win, gathered, hot, part, precv, coll) = scratch[:10]
    views = scratch[10 : 10 + dims["chunks"]]
    (
        chunk_sem,
        t_local,
        t_send,
        t_recv,
        t_side_send,
        t_side_recv,
        r_own_send,
        r_pass_send,
        r_recv,
        r_y_send,
        r_y_recv,
        l_send,
        l_recv,
        l_y_send,
        l_y_recv,
        h_send,
        h_recv,
        p_send,
        p_recv,
        c_send,
        c_recv,
    ) = scratch[10 + dims["chunks"] :]
    line, ways, pieces, subs = dims["line"], dims["ways"], dims["pieces"], dims["subs"]
    chunks, bricks = dims["chunks"], 2 * dims["line"]
    local_modes, depth, width = tensor_ref.shape
    species, cells, _ = coeffs_ref.shape
    modes = local_modes * 2 * ways
    step = local_modes // pieces
    share = cells // ways
    sub = share // subs
    slab = 2 * depth
    layers = cells // PLANE
    per_share = share // PLANE

    g = lax.axis_index("grp")
    b = lax.axis_index("brick")
    x, y = lax.rem(g, 2), lax.div(g, 2)
    z, c = lax.div(b, 2), lax.rem(b, 2)
    other = 1 - c
    nearest = [sorted((q for q in range(line) if q != p), key=lambda q: (abs(q - p), q)) for p in range(line)]
    source = [z] + [lookup([nearest[p][n] for p in range(line)], z) for n in range(line - 1)]
    late = []

    def remote(src, dst, send, recv, tg, tb, when=None):
        copy = pltpu.make_async_remote_copy(
            src_ref=src, dst_ref=dst, send_sem=send, recv_sem=recv, device_id=(tg, tb), device_id_type=MESH
        )
        if when is None:
            copy.start()
        else:
            pl.when(when)(copy.start)
        late.append((copy, when))

    def arrived(dst, recv):
        pltpu.make_async_remote_copy(
            src_ref=dst, dst_ref=dst, send_sem=recv, recv_sem=recv, device_id=(g, b), device_id_type=MESH
        ).wait_recv()

    def share_at(j):
        return lax.rem(y + j, ways)

    for q in range(pieces):
        remote(
            tensor_ref.at[pl.ds(q * step, step)], tbuf.at[x, q, c], t_send.at[q], t_recv.at[q], 2 * y + 1 - x, b
        )
    loads = []
    for j in range(chunks):
        row = pl.multiple_of(share_at(j // per_share) * share + (j % per_share) * PLANE, PLANE)
        copy = pltpu.make_async_copy(coeffs_ref.at[:, pl.ds(row, PLANE)], views[j], chunk_sem.at[j])
        copy.start()
        loads.append(copy)
    own_tensor = []
    for q in range(pieces):
        copy = pltpu.make_async_copy(tensor_ref.at[pl.ds(q * step, step)], tbuf.at[x, q, c], t_local.at[q])
        copy.start()
        own_tensor.append(copy)
        remote(
            tensor_ref.at[pl.ds(q * step, step)],
            tbuf.at[x, q, c],
            t_side_send.at[0, q],
            t_side_recv.at[0, q],
            g,
            2 * z + other,
        )

    receiver, partner = pairs_ref[x, 0], pairs_ref[x, 1]

    for j in range(chunks):
        loads[j].wait()
        if j < per_share:
            part_subs = PLANE // sub
            rbuf[z, y, j * PLANE : (j + 1) * PLANE] = views[j][partner]
            for s in range(j * part_subs, (j + 1) * part_subs):
                rows = pl.ds(s * sub, sub)
                for d, to in enumerate((z - 1, z + 1)):
                    remote(
                        rbuf.at[z, y, rows],
                        rbuf.at[z, y, rows],
                        r_own_send.at[d, s],
                        r_recv.at[z, s],
                        g,
                        2 * to + c,
                        when=(to >= 0) & (to < line),
                    )
        else:
            rbuf[z, share_at(j // per_share), (j % per_share) * PLANE : (j % per_share + 1) * PLANE] = views[j][
                partner
            ]
    for j in range(chunks):
        turned = views[j][receiver].T
        lanes = slice((j % per_share) * PLANE, (j % per_share + 1) * PLANE)
        own_left[:, share_at(j // per_share), :, lanes] = turned.reshape(line, slab, PLANE)
        if j == per_share - 1:
            for n in range(1, line):
                to = source[n]
                remote(own_left.at[to, y], lbuf.at[z, y], l_send.at[n], l_recv.at[z], g, 2 * to + c)
    lbuf[z] = own_left[z]

    wide = -(-modes // PLANE) * PLANE
    for j in range(chunks):
        layer = 1 + share_at(j // per_share) * per_share + j % per_share
        for s in range(species):
            turned = views[j][s, :, :wide].astype(jnp.float32).T
            win[layer, :, s, :] = turned[:modes]
    hot[...] = (lax.broadcasted_iota(jnp.int32, (cells, cells), 0) == lateral_ref[...]).astype(jnp.bfloat16)
    flat = jnp.concatenate(
        [win[1 + i].reshape(modes * species, PLANE).astype(jnp.bfloat16) for i in range(layers)], axis=1
    )
    gathered[...] = jnp.dot(flat, hot[...], preferred_element_type=jnp.float32).reshape(modes, species, cells)
    before, after = lax.rem(b + bricks - 1, bricks), lax.rem(b + 1, bricks)
    remote(win.at[1], win.at[layers + 1], h_send.at[0], h_recv.at[0], g, before)
    remote(win.at[layers], win.at[0], h_send.at[1], h_recv.at[1], g, after)

    def contract(gx, q, zi, yh):
        inner = lax.dot_general(
            tbuf[gx, q].reshape(slab * step, width),
            rbuf[zi, yh],
            (((1,), (1,)), ((), ())),
            preferred_element_type=jnp.float32,
        )
        factor = lbuf[zi, yh].astype(jnp.float32).reshape(2, 1, depth, share)
        terms = inner.reshape(2, step, depth, share) * factor
        sums = jnp.sum(jnp.sum(terms, axis=2), axis=0)
        old = part[zi, gx, yh]
        spots = lax.broadcasted_iota(jnp.int32, old.shape, 0)
        for m in range(step):
            old = jnp.where(spots == q * step + m, sums[m : m + 1], old)
        part[zi, gx, yh] = old

    def block(gx, q_from, q_to, n, j):
        def body(q, carry):
            contract(gx, q, source[n], share_at(j))
            return carry

        lax.fori_loop(q_from, q_to, body, 0)

    ready, pending = [], []

    def run(most):
        for _ in range(min(most, len(pending))):
            pending.pop(0)()

    def rows_ready(n, j):
        pending.append(lambda: block(x, 0, pieces, n, j))
        for q in got:
            pending.append(lambda q=q: block(1 - x, q, q + 1, n, j))
        ready.append((n, j))

    got = []

    def tensor_event(q):
        arrived(tbuf.at[1 - x, q, c], t_recv.at[q])
        remote(
            tbuf.at[1 - x, q, c], tbuf.at[1 - x, q, c], t_side_send.at[1, q], t_side_recv.at[1, q], g, 2 * z + other
        )

    def tensor_ready(q):
        arrived(tbuf.at[1 - x, q, other], t_side_recv.at[1, q])
        for n, j in ready:
            pending.append(lambda n=n, j=j: block(1 - x, q, q + 1, n, j))
        got.append(q)

    def rows_event(n, s):
        src, rows = source[n], pl.ds(s * sub, sub)
        piece = rbuf.at[src, y, rows]
        arrived(piece, r_recv.at[src, s])
        to = jnp.where(src < z, z + 1, z - 1)
        remote(
            piece, piece, r_pass_send.at[n, s], r_recv.at[src, s], g, 2 * to + c, when=(to >= 0) & (to < line)
        )
        for j in range(1, ways):
            remote(piece, piece, r_y_send.at[n, s, j], r_y_recv.at[src, y, s], 2 * share_at(j) + x, b)

    def left_event(n):
        src = source[n]
        arrived(lbuf.at[src, y], l_recv.at[src])
        for j in range(1, ways):
            remote(lbuf.at[src, y], lbuf.at[src, y], l_y_send.at[n, j], l_y_recv.at[src, y], 2 * share_at(j) + x, b)

    def side_event(n, j):
        src, yh = source[n], share_at(j)
        for s in range(subs):
            arrived(rbuf.at[src, yh, pl.ds(s * sub, sub)], r_y_recv.at[src, yh, s])
        arrived(lbuf.at[src, yh], l_y_recv.at[src, yh])

    for copy in own_tensor:
        copy.wait()
    for q in range(pieces):
        arrived(tbuf.at[x, q, other], t_side_recv.at[0, q])
    for j in range(ways):
        rows_ready(0, j)
    run(1)

    events = (line - 1) * subs
    marks = {}
    for q in range(pieces):
        marks.setdefault(min(((q + 1) * events) // pieces, events), []).append(q)
    count = 0
    waiting = []
    for n in range(1, line):
        for s in range(subs):
            rows_event(n, s)
            run(1)
            count += 1
            for q in marks.get(count, []) if count < events else []:
                tensor_event(q)
                run(1)
                tensor_ready(q)
            if s == subs // 2 and waiting:
                for m, j in waiting:
                    side_event(m, j)
                    rows_ready(m, j)
                waiting = []
        left_event(n)
        rows_ready(n, 0)
        waiting = [(n, j) for j in range(1, ways)]
        run(2)
    for q in marks[events]:
        tensor_event(q)
    run(2 * ways)
    for q in marks[events]:
        tensor_ready(q)
    run(len(pending) // 2)
    for m, j in waiting:
        side_event(m, j)
        rows_ready(m, j)
    run(len(pending))

    for n in range(line - 1, 0, -1):
        to = source[n]
        remote(part.at[to], precv.at[z], p_send.at[n], p_recv.at[z], g, 2 * to + c)
    total = part[z]
    for n in range(1, line):
        arrived(precv.at[source[n]], p_recv.at[source[n]])
        total = total + precv[source[n]]
    for gx in range(2):
        for yh in range(ways):
            for i in range(per_share):
                coll[x, y, 1 + yh * per_share + i, gx * local_modes : (gx + 1) * local_modes, :] = total[
                    gx, yh, :, i * PLANE : (i + 1) * PLANE
                ]
    for j in range(2 * ways):
        to = lax.rem(g + j, 2 * ways)
        if j:
            block_ref = coll.at[x, y, pl.ds(1, layers)]
            remote(block_ref, block_ref, c_send.at[0, j], c_recv.at[0, g], to, b)
        remote(coll.at[x, y, 1], coll.at[x, y, layers + 1], c_send.at[1, j], c_recv.at[1, g], to, before)
        remote(coll.at[x, y, layers], coll.at[x, y, 0], c_send.at[2, j], c_recv.at[2, g], to, after)

    arrived(win.at[layers + 1], h_recv.at[0])
    arrived(win.at[0], h_recv.at[1])
    for j in range(2 * ways):
        src = lax.rem(g + j, 2 * ways)
        sx, sy = lax.rem(src, 2), lax.div(src, 2)
        if j:
            arrived(coll.at[sx, sy, pl.ds(1, layers)], c_recv.at[0, src])
        arrived(coll.at[sx, sy, layers + 1], c_recv.at[1, src])
        arrived(coll.at[sx, sy, 0], c_recv.at[2, src])
    for copy, when in late:
        if when is None:
            copy.wait_send()
        else:
            pl.when(when)(copy.wait_send)

    line_of = lax.broadcasted_iota(jnp.int32, (species, PLANE), 0)
    thermo = jnp.zeros((species, PLANE), jnp.float32)
    for s in range(species):
        thermo = jnp.where(line_of == s, thermal_ref[s], thermo)
    chosen = [(line_of == pairs_ref[p, 0]).astype(jnp.float32) for p in range(2)]
    group = 2 * local_modes
    rows = jnp.concatenate(
        [coll[:, :, 1 + i].reshape(2 * ways * group, PLANE) for i in range(layers)], axis=1
    )
    top = rows.astype(jnp.bfloat16)
    rest = rows - top.astype(jnp.float32)
    mid = rest.astype(jnp.bfloat16)
    low = (rest - mid.astype(jnp.float32)).astype(jnp.bfloat16)
    beside = jnp.dot(jnp.concatenate([low, mid, top], axis=0), hot[...], preferred_element_type=jnp.float32)
    count = 2 * ways * group
    beside = beside[:count] + beside[count : 2 * count] + beside[2 * count :]
    zero = jnp.zeros((species, PLANE), jnp.float32)

    def state_of(k):
        if k < 0 or k >= modes:
            return [zero] * (layers + 2)
        out = []
        for i in range(layers + 2):
            add = zero
            for p in range(2):
                add = add + chosen[p] * coll[p, k // group, i, k % group : k % group + 1, :]
            out.append(win[i, k] + collision_update * add)
        return out

    below, middle = state_of(-1), state_of(0)
    for k in range(modes):
        above = state_of(k + 1)
        speed = [
            thermo * (math.sqrt(k) * below[i] + math.sqrt(k + 1.0) * above[i]) for i in range(layers + 2)
        ]
        face = [
            0.5 * (speed[i] + speed[i + 1]) - 0.5 * max_speed * thermo * (middle[i + 1] - middle[i])
            for i in range(layers + 1)
        ]
        for i in range(layers):
            lanes = slice(i * PLANE, (i + 1) * PLANE)
            add = zero
            for p in range(2):
                row = p * ways * group + k
                add = add + chosen[p] * beside[row : row + 1, lanes]
            partner_state = gathered[k, :, lanes] + collision_update * add
            center = middle[i + 1]
            o_ref[k, :, lanes] = (
                center - courant * (face[i + 1] - face[i]) + mixing * (partner_state - center)
            )
        below, middle = middle, above


def local(coeffs, tensor, pairs, lateral, thermal):
    species, cells, width = coeffs.shape
    local_modes, depth, _ = tensor.shape
    bricks, groups = lax.axis_size("brick"), lax.axis_size("grp")
    assert pairs.shape[0] == 2 and bricks % 2 == 0 and groups % 2 == 0
    line, ways = bricks // 2, groups // 2
    modes = local_modes * groups
    share = cells // ways
    assert share % PLANE == 0 and width == bricks * depth
    step = 2 if local_modes % 2 == 0 else 1
    pieces = local_modes // step
    subs = share // 64
    chunks = cells // PLANE
    layers = cells // PLANE
    slab = 2 * depth
    dims = dict(line=line, ways=ways, pieces=pieces, subs=subs, chunks=chunks)
    bf16, f32 = jnp.bfloat16, jnp.float32
    sem = pltpu.SemaphoreType.DMA
    scratch = [
        pltpu.VMEM((2, pieces, 2, step, depth, width), bf16),
        pltpu.VMEM((line, ways, share, width), bf16),
        pltpu.VMEM((line, ways, slab, share), bf16),
        pltpu.VMEM((line, ways, slab, share), bf16),
        pltpu.VMEM((layers + 2, modes, species, PLANE), f32),
        pltpu.VMEM((modes, species, cells), f32),
        pltpu.VMEM((cells, cells), bf16),
        pltpu.VMEM((line, 2, ways, local_modes, share), f32),
        pltpu.VMEM((line, 2, ways, local_modes, share), f32),
        pltpu.VMEM((2, ways, layers + 2, 2 * local_modes, PLANE), f32),
    ]
    scratch += [pltpu.VMEM((species, PLANE, width), bf16)] * chunks
    scratch += [
        sem((chunks,)),
        sem((pieces,)),
        sem((pieces,)),
        sem((pieces,)),
        sem((2, pieces)),
        sem((2, pieces)),
        sem((2, subs)),
        sem((line, subs)),
        sem((line, subs)),
        sem((line, subs, ways)),
        sem((line, ways, subs)),
        sem((line,)),
        sem((line,)),
        sem((line, ways)),
        sem((line, ways)),
        sem((2,)),
        sem((2,)),
        sem((line,)),
        sem((line,)),
        sem((3, groups)),
        sem((3, groups)),
    ]
    return pl.pallas_call(
        lambda *refs: fused_kernel(dims, *refs),
        out_shape=jax.ShapeDtypeStruct((modes, species, cells), f32),
        in_specs=[
            pl.BlockSpec(memory_space=pl.ANY),
            pl.BlockSpec(memory_space=pl.ANY),
            pl.BlockSpec(memory_space=pltpu.VMEM),
            pl.BlockSpec(memory_space=pltpu.SMEM),
            pl.BlockSpec(memory_space=pltpu.SMEM),
        ],
        out_specs=pl.BlockSpec(memory_space=pltpu.VMEM),
        scratch_shapes=scratch,
        compiler_params=pltpu.CompilerParams(has_side_effects=True, vmem_limit_bytes=60 * 2**20),
        name="fused",
    )(coeffs, tensor, lateral.reshape(1, cells), pairs, thermal)


def solution(mesh):
    in_specs = (P(None, "brick", None), P("grp", "brick", None), P(), P("brick"), P())
    out_specs = P(None, None, "brick")
    return jax.shard_map(local, mesh=mesh, in_specs=in_specs, out_specs=out_specs, check_vma=False)
```

```python
import math

import jax
import jax.numpy as jnp
from jax import lax
from jax.experimental import pallas as pl
from jax.experimental.pallas import tpu as pltpu
from jax.sharding import PartitionSpec as P

PLANE = 128

collision_update = 0.5
courant = 0.08
max_speed = 11.0
mixing = 0.2

MESH = pl.DeviceIdType.MESH


def lookup(table, index):
    out = jnp.int32(table[0])
    for i in range(1, len(table)):
        out = jnp.where(index == i, jnp.int32(table[i]), out)
    return out


def fused_kernel(dims, coeffs_ref, tensor_ref, lateral_ref, pairs_ref, thermal_ref, o_ref, *scratch):
    (tbuf, rbuf, lbuf, own_left, win, gathered, hot, part, precv, coll) = scratch[:10]
    views = scratch[10 : 10 + dims["chunks"]]
    (
        chunk_sem,
        t_local,
        t_send,
        t_recv,
        t_side_send,
        t_side_recv,
        r_own_send,
        r_pass_send,
        r_recv,
        r_y_send,
        r_y_recv,
        l_send,
        l_recv,
        l_y_send,
        l_y_recv,
        h_send,
        h_recv,
        p_send,
        p_recv,
        c_send,
        c_recv,
    ) = scratch[10 + dims["chunks"] :]
    line, ways, pieces, subs = dims["line"], dims["ways"], dims["pieces"], dims["subs"]
    chunks, bricks = dims["chunks"], 2 * dims["line"]
    local_modes, depth, width = tensor_ref.shape
    species, cells, _ = coeffs_ref.shape
    modes = local_modes * 2 * ways
    step = local_modes // pieces
    share = cells // ways
    sub = width // subs
    slab = 2 * depth
    layers = cells // PLANE
    per_share = share // PLANE

    g = lax.axis_index("grp")
    b = lax.axis_index("brick")
    x, y = lax.rem(g, 2), lax.div(g, 2)
    z, c = lax.div(b, 2), lax.rem(b, 2)
    other = 1 - c
    nearest = [sorted((q for q in range(line) if q != p), key=lambda q: (abs(q - p), q)) for p in range(line)]
    source = [z] + [lookup([nearest[p][n] for p in range(line)], z) for n in range(line - 1)]
    away = [jnp.abs(source[n] - z) for n in range(line)]
    gaps = [sorted({abs(nearest[p][n - 1] - p) for p in range(line)}) if n else [0] for n in range(line)]
    late = []

    def remote(src, dst, send, recv, tg, tb, when=None):
        copy = pltpu.make_async_remote_copy(
            src_ref=src, dst_ref=dst, send_sem=send, recv_sem=recv, device_id=(tg, tb), device_id_type=MESH
        )
        if when is None:
            copy.start()
        else:
            pl.when(when)(copy.start)
        late.append((copy, when))

    def arrived(dst, recv):
        pltpu.make_async_remote_copy(
            src_ref=dst, dst_ref=dst, send_sem=recv, recv_sem=recv, device_id=(g, b), device_id_type=MESH
        ).wait_recv()

    def share_at(j):
        return lax.rem(y + j, ways)

    before, after = lax.rem(b + bricks - 1, bricks), lax.rem(b + 1, bricks)
    loads = []
    for j in range(chunks):
        row = pl.multiple_of(share_at(j // per_share) * share + (j % per_share) * PLANE, PLANE)
        loads.append(pltpu.make_async_copy(coeffs_ref.at[:, pl.ds(row, PLANE)], views[j], chunk_sem.at[j]))
    for j in range(per_share):
        loads[j].start()
    barrier = pltpu.get_barrier_semaphore()
    peers = [(lax.rem(g + j, 2 * ways), b) for j in range(1, 2 * ways)]
    peers += [(lax.rem(g + j, 2 * ways), to) for j in range(2 * ways) for to in (before, after)]
    peers += [(g, 2 * source[n] + c) for n in range(1, line)]
    for peer in peers:
        pl.semaphore_signal(barrier, inc=1, device_id=peer, device_id_type=MESH)
    pl.semaphore_wait(barrier, len(peers))

    for q in range(pieces):
        remote(
            tensor_ref.at[pl.ds(q * step, step)], tbuf.at[x, q, c], t_send.at[q], t_recv.at[q], 2 * y + 1 - x, b
        )
    own_tensor = []
    for q in range(pieces):
        own_tensor.append(
            pltpu.make_async_copy(tensor_ref.at[pl.ds(q * step, step)], tbuf.at[x, q, c], t_local.at[q])
        )
        remote(
            tensor_ref.at[pl.ds(q * step, step)],
            tbuf.at[x, q, c],
            t_side_send.at[0, q],
            t_side_recv.at[0, q],
            g,
            2 * z + other,
        )

    receiver, partner = pairs_ref[x, 0], pairs_ref[x, 1]

    def lanes_of(j):
        return slice((j % per_share) * PLANE, (j % per_share + 1) * PLANE)

    def turn_rows(j, s):
        span = slice(s * sub, (s + 1) * sub)
        rbuf[z, share_at(j // per_share), span, lanes_of(j)] = views[j][partner, :, span].T

    def turn_left(j):
        own_left[:, share_at(j // per_share), :, lanes_of(j)] = views[j][receiver].T.reshape(line, slab, PLANE)

    for j in range(per_share):
        loads[j].wait()
    for copy in loads[per_share:] + own_tensor:
        copy.start()
    lead = subs // 2
    slots = [lead + (n - 1) * (subs - lead) // (line - 1) for n in range(1, line)]
    for s in range(subs):
        for j in range(per_share):
            turn_rows(j, s)
        if s == lead:
            for j in range(per_share):
                turn_left(j)
        for n in range(1, line):
            if slots[n - 1] == s:
                to = 2 * source[n] + c
                remote(own_left.at[source[n], y], lbuf.at[z, y], l_send.at[n], l_recv.at[z], g, to)
        piece = rbuf.at[z, y, pl.ds(s * sub, sub)]
        for d, to in enumerate((z - 1, z + 1)):
            remote(
                piece, piece, r_own_send.at[d, s], r_recv.at[z, s], g, 2 * to + c, when=(to >= 0) & (to < line)
            )

    def other_shares():
        for j in range(per_share, chunks):
            loads[j].wait()
            for s in range(subs):
                turn_rows(j, s)
            turn_left(j)
        lbuf[z] = own_left[z]

    wide = -(-modes // PLANE) * PLANE

    def window_task(j):
        layer = 1 + share_at(j // per_share) * per_share + j % per_share
        for s in range(species):
            turned = views[j][s, :, :wide].astype(jnp.float32).T
            win[layer, :, s, :] = turned[:modes]

    def lateral_task():
        hot[...] = (lax.broadcasted_iota(jnp.int32, (cells, cells), 0) == lateral_ref[...]).astype(jnp.bfloat16)
        flat = jnp.concatenate(
            [win[1 + i].reshape(modes * species, PLANE).astype(jnp.bfloat16) for i in range(layers)], axis=1
        )
        gathered[...] = jnp.dot(flat, hot[...], preferred_element_type=jnp.float32).reshape(modes, species, cells)

    def halo_task():
        remote(win.at[1], win.at[layers + 1], h_send.at[0], h_recv.at[0], g, before)
        remote(win.at[layers], win.at[0], h_send.at[1], h_recv.at[1], g, after)

    def contract(gx, q, count, zi, yh):
        halves = []
        for half in range(2):
            inner = jnp.dot(
                tbuf[gx, pl.ds(q, count), half].reshape(count * step * depth, width),
                rbuf[zi, yh],
                preferred_element_type=jnp.float32,
            )
            factor = lbuf[zi, yh, half * depth : (half + 1) * depth].astype(jnp.float32)
            terms = inner.reshape(count * step, depth, share) * factor[None]
            halves.append(jnp.sum(terms, axis=1))
        return halves[0] + halves[1]

    def block(gx, q, count, n, j):
        zi, yh = source[n], share_at(j)
        part[zi, gx, yh, q * step : (q + count) * step, :] = contract(gx, q, count, zi, yh)

    done = {}

    def finished(kind, n, j, count):
        done[kind, n, j] = done.get((kind, n, j), 0) + count
        if n and done[kind, n, j] == pieces:
            gx, yh, to = (x, 1 - x)[kind], share_at(j), source[n]
            remote(part.at[to, gx, yh], precv.at[z, gx, yh], p_send.at[n, kind, j], p_recv.at[z, gx, yh], g, 2 * to + c)

    def work(kind, q, count, n, j):
        def go():
            block((x, 1 - x)[kind], q, count, n, j)
            finished(kind, n, j, count)

        return (count * 0.09 + 0.06, go)

    wire = 92e3
    piece_us = 2 * share * width * 2 / wire
    left_us = 2 * slab * share * 2 / wire
    tensor_us = 2 * step * depth * width * 2 / wire
    begin, hop, side_hop = 0.7, 2.6, 3.4
    sub_us = piece_us / subs
    agenda = []
    for n in range(1, line):
        left_at = begin + slots[n - 1] * sub_us + 2 * n * left_us
        agenda.append((left_at, "left", n, 0, 0))
        last = 0.0
        for gap in gaps[n]:
            for s in range(subs):
                at = begin + (gap - 1) * piece_us + (s + 1) * sub_us
                if gap == 1:
                    at += left_us * sum(s >= slot for slot in slots[:2])
                elif gap == 2:
                    at += left_us * (2 + (line - 3) * (s + 1) / subs)
                else:
                    at += left_us * (line - 1)
                agenda.append((at, "rows", n, s, gap))
            last = at
        agenda.append((max(last, left_at) + 0.01, "own", n, 0, 0))
        for j in range(1, ways):
            agenda.append((max(last, left_at) + sub_us + hop + 2.0, "side", n, j, 0))
    for q in range(pieces):
        agenda.append((hop + (q + 1) * tensor_us, "tensor", q, 0, 0))
        agenda.append((hop + (q + 1) * tensor_us + side_hop, "tensor_side", q, 0, 0))
    agenda.sort(key=lambda item: item[0])

    pending, got, ready = [], [], []
    half = max(1, pieces // 2)

    def rows_ready(n, j):
        for q in range(0, pieces, half):
            pending.append(work(0, q, half, n, j))
        run_from = 0
        while run_from < len(got):
            count = min(half, len(got) - run_from)
            pending.append(work(1, run_from, count, n, j))
            run_from += count
        ready.append((n, j))

    def tensor_event(q):
        arrived(tbuf.at[1 - x, q, c], t_recv.at[q])
        remote(
            tbuf.at[1 - x, q, c], tbuf.at[1 - x, q, c], t_side_send.at[1, q], t_side_recv.at[1, q], g, 2 * z + other
        )

    def tensor_ready(q):
        arrived(tbuf.at[1 - x, q, other], t_side_recv.at[1, q])
        for n, j in ready:
            pending.append(work(1, q, 1, n, j))
        got.append(q)

    def rows_event(n, s, gap):
        src = source[n]
        piece = rbuf.at[src, y, pl.ds(s * sub, sub)]
        near = away[n] == gap
        pl.when(near)(lambda: arrived(piece, r_recv.at[src, s]))
        to = jnp.where(src < z, z + 1, z - 1)
        remote(
            piece,
            piece,
            r_pass_send.at[n, s],
            r_recv.at[src, s],
            g,
            2 * to + c,
            when=near & (to >= 0) & (to < line),
        )
        for j in range(1, ways):
            remote(
                piece, piece, r_y_send.at[n, s, j], r_y_recv.at[src, y, s], 2 * share_at(j) + x, b, when=near
            )

    def left_event(n):
        src = source[n]
        arrived(lbuf.at[src, y], l_recv.at[src])
        for j in range(1, ways):
            remote(lbuf.at[src, y], lbuf.at[src, y], l_y_send.at[n, j], l_y_recv.at[src, y], 2 * share_at(j) + x, b)

    def side_event(n, j):
        src, yh = source[n], share_at(j)
        for s in range(subs):
            arrived(rbuf.at[src, yh, pl.ds(s * sub, sub)], r_y_recv.at[src, yh, s])
        arrived(lbuf.at[src, yh], l_y_recv.at[src, yh])

    def own_side():
        other_shares()
        for copy in own_tensor:
            copy.wait()
        for q in range(pieces):
            arrived(tbuf.at[x, q, other], t_side_recv.at[0, q])
        for j in range(ways):
            rows_ready(0, j)
        for j in range(chunks):
            pending.append((0.5, lambda j=j: window_task(j)))
        pending.append((0.3, halo_task))
        pending.append((1.0, lateral_task))

    clock = 3.0
    agenda.append((clock + 1.0, "own", 0, 0, 0))
    agenda.sort(key=lambda item: item[0])
    for when, what, n, s, gap in agenda:
        while pending and clock + 0.5 * pending[0][0] < when:
            cost, go = pending.pop(0)
            go()
            clock += cost
        clock = max(clock, when)
        if what == "rows":
            rows_event(n, s, gap)
        elif what == "left":
            left_event(n)
        elif what == "side":
            side_event(n, s)
            rows_ready(n, s)
        elif what == "tensor":
            tensor_event(n)
        elif what == "tensor_side":
            tensor_ready(n)
        elif n:
            rows_ready(n, 0)
        else:
            own_side()
    for _, go in pending:
        go()

    arrivals = [(n, kind, j) for n in range(1, line) for kind in range(2) for j in range(ways)]
    for n, kind, j in arrivals:
        spot = precv.at[source[n], (x, 1 - x)[kind], share_at(j)]
        arrived(spot, p_recv.at[source[n], (x, 1 - x)[kind], share_at(j)])
    total = part[z]
    for n in range(1, line):
        total = total + precv[source[n]]
    for gx in range(2):
        for yh in range(ways):
            for i in range(per_share):
                coll[x, y, 1 + yh * per_share + i, gx * local_modes : (gx + 1) * local_modes, :] = total[
                    gx, yh, :, i * PLANE : (i + 1) * PLANE
                ]
    for j in range(2 * ways):
        to = lax.rem(g + j, 2 * ways)
        if j:
            block_ref = coll.at[x, y, pl.ds(1, layers)]
            remote(block_ref, block_ref, c_send.at[0, j], c_recv.at[0, g], to, b)
        remote(coll.at[x, y, 1], coll.at[x, y, layers + 1], c_send.at[1, j], c_recv.at[1, g], to, before)
        remote(coll.at[x, y, layers], coll.at[x, y, 0], c_send.at[2, j], c_recv.at[2, g], to, after)

    arrived(win.at[layers + 1], h_recv.at[0])
    arrived(win.at[0], h_recv.at[1])
    for j in range(2 * ways):
        src = lax.rem(g + j, 2 * ways)
        sx, sy = lax.rem(src, 2), lax.div(src, 2)
        if j:
            arrived(coll.at[sx, sy, pl.ds(1, layers)], c_recv.at[0, src])
        arrived(coll.at[sx, sy, layers + 1], c_recv.at[1, src])
        arrived(coll.at[sx, sy, 0], c_recv.at[2, src])
    for copy, when in late:
        if when is None:
            copy.wait_send()
        else:
            pl.when(when)(copy.wait_send)

    line_of = lax.broadcasted_iota(jnp.int32, (species, PLANE), 0)
    thermo = jnp.zeros((species, PLANE), jnp.float32)
    for s in range(species):
        thermo = jnp.where(line_of == s, thermal_ref[s], thermo)
    chosen = [(line_of == pairs_ref[p, 0]).astype(jnp.float32) for p in range(2)]
    group = 2 * local_modes
    rows = jnp.concatenate(
        [coll[:, :, 1 + i].reshape(2 * ways * group, PLANE) for i in range(layers)], axis=1
    )
    top = rows.astype(jnp.bfloat16)
    rest = rows - top.astype(jnp.float32)
    mid = rest.astype(jnp.bfloat16)
    low = (rest - mid.astype(jnp.float32)).astype(jnp.bfloat16)
    beside = jnp.dot(jnp.concatenate([low, mid, top], axis=0), hot[...], preferred_element_type=jnp.float32)
    count = 2 * ways * group
    beside = beside[:count] + beside[count : 2 * count] + beside[2 * count :]
    zero = jnp.zeros((species, PLANE), jnp.float32)

    def state_of(k):
        if k < 0 or k >= modes:
            return [zero] * (layers + 2)
        out = []
        for i in range(layers + 2):
            add = zero
            for p in range(2):
                add = add + chosen[p] * coll[p, k // group, i, k % group : k % group + 1, :]
            out.append(win[i, k] + collision_update * add)
        return out

    below, middle = state_of(-1), state_of(0)
    for k in range(modes):
        above = state_of(k + 1)
        speed = [
            thermo * (math.sqrt(k) * below[i] + math.sqrt(k + 1.0) * above[i]) for i in range(layers + 2)
        ]
        face = [
            0.5 * (speed[i] + speed[i + 1]) - 0.5 * max_speed * thermo * (middle[i + 1] - middle[i])
            for i in range(layers + 1)
        ]
        for i in range(layers):
            lanes = slice(i * PLANE, (i + 1) * PLANE)
            add = zero
            for p in range(2):
                row = p * ways * group + k
                add = add + chosen[p] * beside[row : row + 1, lanes]
            partner_state = gathered[k, :, lanes] + collision_update * add
            center = middle[i + 1]
            o_ref[k, :, lanes] = (
                center - courant * (face[i + 1] - face[i]) + mixing * (partner_state - center)
            )
        below, middle = middle, above


def local(coeffs, tensor, pairs, lateral, thermal):
    species, cells, width = coeffs.shape
    local_modes, depth, _ = tensor.shape
    bricks, groups = lax.axis_size("brick"), lax.axis_size("grp")
    assert pairs.shape[0] == 2 and bricks % 2 == 0 and groups % 2 == 0
    line, ways = bricks // 2, groups // 2
    modes = local_modes * groups
    share = cells // ways
    assert share % PLANE == 0 and width == bricks * depth
    step = 1
    pieces = local_modes // step
    subs = width // PLANE
    chunks = cells // PLANE
    layers = cells // PLANE
    slab = 2 * depth
    dims = dict(line=line, ways=ways, pieces=pieces, subs=subs, chunks=chunks)
    bf16, f32 = jnp.bfloat16, jnp.float32
    sem = pltpu.SemaphoreType.DMA
    scratch = [
        pltpu.VMEM((2, pieces, 2, step, depth, width), bf16),
        pltpu.VMEM((line, ways, width, share), bf16),
        pltpu.VMEM((line, ways, slab, share), bf16),
        pltpu.VMEM((line, ways, slab, share), bf16),
        pltpu.VMEM((layers + 2, modes, species, PLANE), f32),
        pltpu.VMEM((modes, species, cells), f32),
        pltpu.VMEM((cells, cells), bf16),
        pltpu.VMEM((line, 2, ways, local_modes, share), f32),
        pltpu.VMEM((line, 2, ways, local_modes, share), f32),
        pltpu.VMEM((2, ways, layers + 2, 2 * local_modes, PLANE), f32),
    ]
    scratch += [pltpu.VMEM((species, PLANE, width), bf16)] * chunks
    scratch += [
        sem((chunks,)),
        sem((pieces,)),
        sem((pieces,)),
        sem((pieces,)),
        sem((2, pieces)),
        sem((2, pieces)),
        sem((2, subs)),
        sem((line, subs)),
        sem((line, subs)),
        sem((line, subs, ways)),
        sem((line, ways, subs)),
        sem((line,)),
        sem((line,)),
        sem((line, ways)),
        sem((line, ways)),
        sem((2,)),
        sem((2,)),
        sem((line, 2, ways)),
        sem((line, 2, ways)),
        sem((3, groups)),
        sem((3, groups)),
    ]
    return pl.pallas_call(
        lambda *refs: fused_kernel(dims, *refs),
        out_shape=jax.ShapeDtypeStruct((modes, species, cells), f32),
        in_specs=[
            pl.BlockSpec(memory_space=pl.ANY),
            pl.BlockSpec(memory_space=pl.ANY),
            pl.BlockSpec(memory_space=pltpu.VMEM),
            pl.BlockSpec(memory_space=pltpu.SMEM),
            pl.BlockSpec(memory_space=pltpu.SMEM),
        ],
        out_specs=pl.BlockSpec(memory_space=pltpu.VMEM),
        scratch_shapes=scratch,
        compiler_params=pltpu.CompilerParams(has_side_effects=True, collective_id=0, vmem_limit_bytes=60 * 2**20),
        name="fused",
    )(coeffs, tensor, lateral.reshape(1, cells), pairs, thermal)


def solution(mesh):
    in_specs = (P(None, "brick", None), P("grp", "brick", None), P(), P("brick"), P())
    out_specs = P(None, None, "brick")
    return jax.shard_map(local, mesh=mesh, in_specs=in_specs, out_specs=out_specs, check_vma=False)
```

```python
import math

import jax
import jax.numpy as jnp
from jax import lax
from jax.experimental import pallas as pl
from jax.experimental.pallas import tpu as pltpu
from jax.sharding import PartitionSpec as P

PLANE = 128

collision_update = 0.5
courant = 0.08
max_speed = 11.0
mixing = 0.2

MESH = pl.DeviceIdType.MESH


def lookup(table, index):
    out = jnp.int32(table[0])
    for i in range(1, len(table)):
        out = jnp.where(index == i, jnp.int32(table[i]), out)
    return out


def fused_kernel(dims, coeffs_ref, tensor_ref, lateral_ref, pairs_ref, thermal_ref, o_ref, *scratch):
    (tbuf, rbuf, lbuf, own_left, win, gathered, hot, part, precv, coll, edge, rim) = scratch[:12]
    views = scratch[12 : 12 + dims["chunks"]]
    (
        chunk_sem,
        t_local,
        t_send,
        t_recv,
        t_side_send,
        t_side_recv,
        r_own_send,
        r_pass_send,
        r_recv,
        r_y_send,
        r_y_recv,
        l_send,
        l_recv,
        l_y_send,
        l_y_recv,
        h_send,
        h_recv,
        p_send,
        p_recv,
        c_send,
        c_recv,
    ) = scratch[12 + dims["chunks"] :]
    line, ways, pieces, subs = dims["line"], dims["ways"], dims["pieces"], dims["subs"]
    chunks, bricks = dims["chunks"], 2 * dims["line"]
    local_modes, depth, width = tensor_ref.shape
    species, cells, _ = coeffs_ref.shape
    modes = local_modes * 2 * ways
    step = local_modes // pieces
    share = cells // ways
    sub = width // subs
    slab = 2 * depth
    cuts = dims["cuts"]
    cut = slab // cuts
    layers = cells // PLANE
    per_share = share // PLANE

    g = lax.axis_index("grp")
    b = lax.axis_index("brick")
    x, y = lax.rem(g, 2), lax.div(g, 2)
    z, c = lax.div(b, 2), lax.rem(b, 2)
    other = 1 - c
    nearest = [sorted((q for q in range(line) if q != p), key=lambda q: (abs(q - p), q)) for p in range(line)]
    source = [z] + [lookup([nearest[p][n] for p in range(line)], z) for n in range(line - 1)]
    away = [jnp.abs(source[n] - z) for n in range(line)]
    gaps = [sorted({abs(nearest[p][n - 1] - p) for p in range(line)}) if n else [0] for n in range(line)]
    late = []

    def remote(src, dst, send, recv, tg, tb, when=None):
        copy = pltpu.make_async_remote_copy(
            src_ref=src, dst_ref=dst, send_sem=send, recv_sem=recv, device_id=(tg, tb), device_id_type=MESH
        )
        if when is None:
            copy.start()
        else:
            pl.when(when)(copy.start)
        late.append((copy, when))

    def arrived(dst, recv):
        pltpu.make_async_remote_copy(
            src_ref=dst, dst_ref=dst, send_sem=recv, recv_sem=recv, device_id=(g, b), device_id_type=MESH
        ).wait_recv()

    def share_at(j):
        return lax.rem(y + j, ways)

    before, after = lax.rem(b + bricks - 1, bricks), lax.rem(b + 1, bricks)
    loads = []
    for j in range(chunks):
        row = pl.multiple_of(share_at(j // per_share) * share + (j % per_share) * PLANE, PLANE)
        loads.append(pltpu.make_async_copy(coeffs_ref.at[:, pl.ds(row, PLANE)], views[j], chunk_sem.at[j]))
    for j in range(per_share):
        loads[j].start()
    barrier = pltpu.get_barrier_semaphore()
    peers = [(lax.rem(g + j, 2 * ways), b) for j in range(1, 2 * ways)]
    peers += [(lax.rem(g + j, 2 * ways), to) for j in range(2 * ways) for to in (before, after)]
    peers += [(g, 2 * source[n] + c) for n in range(1, line)]
    for peer in peers:
        pl.semaphore_signal(barrier, inc=1, device_id=peer, device_id_type=MESH)
    pl.semaphore_wait(barrier, len(peers))

    for q in range(pieces):
        remote(
            tensor_ref.at[pl.ds(q * step, step)], tbuf.at[x, q, c], t_send.at[q], t_recv.at[q], 2 * y + 1 - x, b
        )
    own_tensor = []
    for q in range(pieces):
        own_tensor.append(
            pltpu.make_async_copy(tensor_ref.at[pl.ds(q * step, step)], tbuf.at[x, q, c], t_local.at[q])
        )
        remote(
            tensor_ref.at[pl.ds(q * step, step)],
            tbuf.at[x, q, c],
            t_side_send.at[0, q],
            t_side_recv.at[0, q],
            g,
            2 * z + other,
        )

    receiver, partner = pairs_ref[x, 0], pairs_ref[x, 1]

    def lanes_of(j):
        return slice((j % per_share) * PLANE, (j % per_share + 1) * PLANE)

    def turn_rows(j, s):
        span = slice(s * sub, (s + 1) * sub)
        rbuf[z, share_at(j // per_share), span, lanes_of(j)] = views[j][partner, :, span].T

    def turn_left(j):
        own_left[:, share_at(j // per_share), :, lanes_of(j)] = views[j][receiver].T.reshape(line, slab, PLANE)

    for j in range(per_share):
        loads[j].wait()
    for copy in loads[per_share:] + own_tensor:
        copy.start()
    lead = subs // 2
    slots = [lead + (n - 1) * (subs - lead) // (line - 1) for n in range(1, line)]
    for s in range(subs):
        for j in range(per_share):
            turn_rows(j, s)
        if s == lead:
            for j in range(per_share):
                turn_left(j)
        for n in range(1, line):
            if slots[n - 1] == s:
                to = 2 * source[n] + c
                for k in range(cuts):
                    span = pl.ds(k * cut, cut)
                    remote(
                        own_left.at[source[n], y, span],
                        lbuf.at[z, y, span],
                        l_send.at[n, k],
                        l_recv.at[z, k],
                        g,
                        to,
                    )
        piece = rbuf.at[z, y, pl.ds(s * sub, sub)]
        for d, to in enumerate((z - 1, z + 1)):
            remote(
                piece, piece, r_own_send.at[d, s], r_recv.at[z, s], g, 2 * to + c, when=(to >= 0) & (to < line)
            )

    def other_shares():
        for j in range(per_share, chunks):
            loads[j].wait()
            for s in range(subs):
                turn_rows(j, s)
            turn_left(j)
        lbuf[z] = own_left[z]

    wide = -(-modes // PLANE) * PLANE

    def window_task(j):
        layer = 1 + share_at(j // per_share) * per_share + j % per_share
        for s in range(species):
            turned = views[j][s, :, :wide].astype(jnp.float32).T
            win[layer, :, s, :] = turned[:modes]

    def lateral_task():
        hot[...] = (lax.broadcasted_iota(jnp.int32, (cells, cells), 0) == lateral_ref[...]).astype(jnp.bfloat16)
        flat = jnp.concatenate(
            [win[1 + i].reshape(modes * species, PLANE).astype(jnp.bfloat16) for i in range(layers)], axis=1
        )
        gathered[...] = jnp.dot(flat, hot[...], preferred_element_type=jnp.float32).reshape(modes, species, cells)

    def halo_task():
        edge[0] = win[1].astype(jnp.bfloat16)
        edge[1] = win[layers].astype(jnp.bfloat16)
        remote(edge.at[0], rim.at[1], h_send.at[0], h_recv.at[1], g, before)
        remote(edge.at[1], rim.at[0], h_send.at[1], h_recv.at[0], g, after)

    def contract(gx, q, count, zi, yh):
        halves = []
        for half in range(2):
            inner = jnp.dot(
                tbuf[gx, pl.ds(q, count), half].reshape(count * step * depth, width),
                rbuf[zi, yh],
                preferred_element_type=jnp.float32,
            )
            factor = lbuf[zi, yh, half * depth : (half + 1) * depth].astype(jnp.float32)
            terms = inner.reshape(count * step, depth, share) * factor[None]
            halves.append(jnp.sum(terms, axis=1))
        return halves[0] + halves[1]

    def block(gx, q, count, n, j):
        zi, yh = source[n], share_at(j)
        part[zi, gx, yh, q * step : (q + count) * step, :] = contract(gx, q, count, zi, yh)

    done = {}

    def finished(kind, n, j, count):
        done[kind, n, j] = done.get((kind, n, j), 0) + count
        if n and done[kind, n, j] == pieces:
            gx, yh, to = (x, 1 - x)[kind], share_at(j), source[n]
            remote(part.at[to, gx, yh], precv.at[z, gx, yh], p_send.at[n, kind, j], p_recv.at[z, gx, yh], g, 2 * to + c)

    def work(kind, q, count, n, j):
        def go():
            block((x, 1 - x)[kind], q, count, n, j)
            finished(kind, n, j, count)

        return (count * 0.09 + 0.06, go)

    wire = 92e3
    piece_us = 2 * share * width * 2 / wire
    left_us = 2 * slab * share * 2 / wire
    tensor_us = 2 * step * depth * width * 2 / wire
    begin, hop, side_hop = 0.7, 2.6, 3.4
    sub_us = piece_us / subs
    agenda = []
    for n in range(1, line):
        left_at = begin + slots[n - 1] * sub_us + 2 * n * left_us + (2.0 if n > 1 else 0.0)
        for k in range(cuts):
            agenda.append((left_at - (cuts - 1 - k) * left_us * 2 / cuts, "left", n, k, 0))
        last = 0.0
        for gap in gaps[n]:
            for s in range(subs):
                at = begin + (gap - 1) * piece_us + (s + 1) * sub_us
                if gap == 1:
                    at += left_us * sum(s >= slot for slot in slots[:1])
                elif gap == 2:
                    at += left_us * (2 + (line - 3) * (s + 1) / subs)
                else:
                    at += left_us * (line - 1)
                agenda.append((at + (1.7 if gap > 1 else 0.0), "rows", n, s, gap))
            last = at + 1.7
        agenda.append((max(last, left_at) + 0.01, "own", n, 0, 0))
        for j in range(1, ways):
            agenda.append((max(last, left_at) + sub_us + hop + 3.0, "side", n, j, 0))
    for q in range(pieces):
        agenda.append((hop + (q + 1) * tensor_us, "tensor", q, 0, 0))
        agenda.append((hop + (q + 1) * tensor_us + side_hop, "tensor_side", q, 0, 0))
    agenda.sort(key=lambda item: item[0])

    pending, got, ready = [], [], []
    half = max(1, pieces // 2)

    def rows_ready(n, j):
        for q in range(0, pieces, half):
            pending.append(work(0, q, half, n, j))
        run_from = 0
        while run_from < len(got):
            count = min(half, len(got) - run_from)
            pending.append(work(1, run_from, count, n, j))
            run_from += count
        ready.append((n, j))

    def tensor_event(q):
        arrived(tbuf.at[1 - x, q, c], t_recv.at[q])
        remote(
            tbuf.at[1 - x, q, c], tbuf.at[1 - x, q, c], t_side_send.at[1, q], t_side_recv.at[1, q], g, 2 * z + other
        )

    def tensor_ready(q):
        arrived(tbuf.at[1 - x, q, other], t_side_recv.at[1, q])
        for n, j in ready:
            pending.append(work(1, q, 1, n, j))
        got.append(q)

    def rows_event(n, s, gap):
        src = source[n]
        piece = rbuf.at[src, y, pl.ds(s * sub, sub)]
        near = away[n] == gap
        pl.when(near)(lambda: arrived(piece, r_recv.at[src, s]))
        to = jnp.where(src < z, z + 1, z - 1)
        remote(
            piece,
            piece,
            r_pass_send.at[n, s],
            r_recv.at[src, s],
            g,
            2 * to + c,
            when=near & (to >= 0) & (to < line),
        )
        for j in range(1, ways):
            remote(
                piece, piece, r_y_send.at[n, s, j], r_y_recv.at[src, y, s], 2 * share_at(j) + x, b, when=near
            )

    def left_event(n, k):
        src = source[n]
        piece = lbuf.at[src, y, pl.ds(k * cut, cut)]
        arrived(piece, l_recv.at[src, k])
        for j in range(1, ways):
            remote(piece, piece, l_y_send.at[n, j, k], l_y_recv.at[src, y, k], 2 * share_at(j) + x, b)

    def side_event(n, j):
        src, yh = source[n], share_at(j)
        for s in range(subs):
            arrived(rbuf.at[src, yh, pl.ds(s * sub, sub)], r_y_recv.at[src, yh, s])
        for k in range(cuts):
            arrived(lbuf.at[src, yh, pl.ds(k * cut, cut)], l_y_recv.at[src, yh, k])

    def own_side():
        other_shares()
        for copy in own_tensor:
            copy.wait()
        for q in range(pieces):
            arrived(tbuf.at[x, q, other], t_side_recv.at[0, q])
        for j in range(ways):
            rows_ready(0, j)
        for j in range(chunks):
            pending.append((0.5, lambda j=j: window_task(j)))
        pending.append((0.3, halo_task))
        pending.append((1.0, lateral_task))

    clock = 3.0
    agenda.append((clock + 1.0, "own", 0, 0, 0))
    agenda.sort(key=lambda item: item[0])
    for when, what, n, s, gap in agenda:
        while pending and clock + 0.5 * pending[0][0] < when:
            cost, go = pending.pop(0)
            go()
            clock += cost
        clock = max(clock, when)
        if what == "rows":
            rows_event(n, s, gap)
        elif what == "left":
            left_event(n, s)
        elif what == "side":
            side_event(n, s)
            rows_ready(n, s)
        elif what == "tensor":
            tensor_event(n)
        elif what == "tensor_side":
            tensor_ready(n)
        elif n:
            rows_ready(n, 0)
        else:
            own_side()
    for _, go in pending:
        go()

    arrivals = [(n, kind, j) for n in range(1, line) for kind in range(2) for j in range(ways)]
    for n, kind, j in arrivals:
        spot = precv.at[source[n], (x, 1 - x)[kind], share_at(j)]
        arrived(spot, p_recv.at[source[n], (x, 1 - x)[kind], share_at(j)])
    total = part[z]
    for n in range(1, line):
        total = total + precv[source[n]]
    for gx in range(2):
        for yh in range(ways):
            for i in range(per_share):
                coll[x, y, 1 + yh * per_share + i, gx * local_modes : (gx + 1) * local_modes, :] = total[
                    gx, yh, :, i * PLANE : (i + 1) * PLANE
                ]
    for j in range(2 * ways):
        to = lax.rem(g + j, 2 * ways)
        if j:
            block_ref = coll.at[x, y, pl.ds(1, layers)]
            remote(block_ref, block_ref, c_send.at[0, j], c_recv.at[0, g], to, b)
        remote(coll.at[x, y, 1], coll.at[x, y, layers + 1], c_send.at[1, j], c_recv.at[1, g], to, before)
        remote(coll.at[x, y, layers], coll.at[x, y, 0], c_send.at[2, j], c_recv.at[2, g], to, after)

    for d in range(2):
        arrived(rim.at[d], h_recv.at[d])
        win[d * (layers + 1)] = rim[d].astype(jnp.float32)
    for j in range(2 * ways):
        src = lax.rem(g + j, 2 * ways)
        sx, sy = lax.rem(src, 2), lax.div(src, 2)
        if j:
            arrived(coll.at[sx, sy, pl.ds(1, layers)], c_recv.at[0, src])
        arrived(coll.at[sx, sy, layers + 1], c_recv.at[1, src])
        arrived(coll.at[sx, sy, 0], c_recv.at[2, src])
    for copy, when in late:
        if when is None:
            copy.wait_send()
        else:
            pl.when(when)(copy.wait_send)

    line_of = lax.broadcasted_iota(jnp.int32, (species, PLANE), 0)
    thermo = jnp.zeros((species, PLANE), jnp.float32)
    for s in range(species):
        thermo = jnp.where(line_of == s, thermal_ref[s], thermo)
    chosen = [(line_of == pairs_ref[p, 0]).astype(jnp.float32) for p in range(2)]
    group = 2 * local_modes
    rows = jnp.concatenate(
        [coll[:, :, 1 + i].reshape(2 * ways * group, PLANE) for i in range(layers)], axis=1
    )
    top = rows.astype(jnp.bfloat16)
    rest = rows - top.astype(jnp.float32)
    mid = rest.astype(jnp.bfloat16)
    low = (rest - mid.astype(jnp.float32)).astype(jnp.bfloat16)
    beside = jnp.dot(jnp.concatenate([low, mid, top], axis=0), hot[...], preferred_element_type=jnp.float32)
    count = 2 * ways * group
    beside = beside[:count] + beside[count : 2 * count] + beside[2 * count :]
    zero = jnp.zeros((species, PLANE), jnp.float32)

    def state_of(k):
        if k < 0 or k >= modes:
            return [zero] * (layers + 2)
        out = []
        for i in range(layers + 2):
            add = zero
            for p in range(2):
                add = add + chosen[p] * coll[p, k // group, i, k % group : k % group + 1, :]
            out.append(win[i, k] + collision_update * add)
        return out

    below, middle = state_of(-1), state_of(0)
    for k in range(modes):
        above = state_of(k + 1)
        speed = [
            thermo * (math.sqrt(k) * below[i] + math.sqrt(k + 1.0) * above[i]) for i in range(layers + 2)
        ]
        face = [
            0.5 * (speed[i] + speed[i + 1]) - 0.5 * max_speed * thermo * (middle[i + 1] - middle[i])
            for i in range(layers + 1)
        ]
        for i in range(layers):
            lanes = slice(i * PLANE, (i + 1) * PLANE)
            add = zero
            for p in range(2):
                row = p * ways * group + k
                add = add + chosen[p] * beside[row : row + 1, lanes]
            partner_state = gathered[k, :, lanes] + collision_update * add
            center = middle[i + 1]
            o_ref[k, :, lanes] = (
                center - courant * (face[i + 1] - face[i]) + mixing * (partner_state - center)
            )
        below, middle = middle, above


def local(coeffs, tensor, pairs, lateral, thermal):
    species, cells, width = coeffs.shape
    local_modes, depth, _ = tensor.shape
    bricks, groups = lax.axis_size("brick"), lax.axis_size("grp")
    assert pairs.shape[0] == 2 and bricks % 2 == 0 and groups % 2 == 0
    line, ways = bricks // 2, groups // 2
    modes = local_modes * groups
    share = cells // ways
    assert share % PLANE == 0 and width == bricks * depth
    step = 1
    pieces = local_modes // step
    subs = width // PLANE
    chunks = cells // PLANE
    layers = cells // PLANE
    slab = 2 * depth
    cuts = 4 if slab % 64 == 0 else 1
    dims = dict(cuts=cuts, line=line, ways=ways, pieces=pieces, subs=subs, chunks=chunks)
    bf16, f32 = jnp.bfloat16, jnp.float32
    sem = pltpu.SemaphoreType.DMA
    scratch = [
        pltpu.VMEM((2, pieces, 2, step, depth, width), bf16),
        pltpu.VMEM((line, ways, width, share), bf16),
        pltpu.VMEM((line, ways, slab, share), bf16),
        pltpu.VMEM((line, ways, slab, share), bf16),
        pltpu.VMEM((layers + 2, modes, species, PLANE), f32),
        pltpu.VMEM((modes, species, cells), f32),
        pltpu.VMEM((cells, cells), bf16),
        pltpu.VMEM((line, 2, ways, local_modes, share), f32),
        pltpu.VMEM((line, 2, ways, local_modes, share), f32),
        pltpu.VMEM((2, ways, layers + 2, 2 * local_modes, PLANE), f32),
        pltpu.VMEM((2, modes, species, PLANE), bf16),
        pltpu.VMEM((2, modes, species, PLANE), bf16),
    ]
    scratch += [pltpu.VMEM((species, PLANE, width), bf16)] * chunks
    scratch += [
        sem((chunks,)),
        sem((pieces,)),
        sem((pieces,)),
        sem((pieces,)),
        sem((2, pieces)),
        sem((2, pieces)),
        sem((2, subs)),
        sem((line, subs)),
        sem((line, subs)),
        sem((line, subs, ways)),
        sem((line, ways, subs)),
        sem((line, cuts)),
        sem((line, cuts)),
        sem((line, ways, cuts)),
        sem((line, ways, cuts)),
        sem((2,)),
        sem((2,)),
        sem((line, 2, ways)),
        sem((line, 2, ways)),
        sem((3, groups)),
        sem((3, groups)),
    ]
    return pl.pallas_call(
        lambda *refs: fused_kernel(dims, *refs),
        out_shape=jax.ShapeDtypeStruct((modes, species, cells), f32),
        in_specs=[
            pl.BlockSpec(memory_space=pl.ANY),
            pl.BlockSpec(memory_space=pl.ANY),
            pl.BlockSpec(memory_space=pltpu.VMEM),
            pl.BlockSpec(memory_space=pltpu.SMEM),
            pl.BlockSpec(memory_space=pltpu.SMEM),
        ],
        out_specs=pl.BlockSpec(memory_space=pltpu.VMEM),
        scratch_shapes=scratch,
        compiler_params=pltpu.CompilerParams(has_side_effects=True, collective_id=0, vmem_limit_bytes=60 * 2**20),
        name="fused",
    )(coeffs, tensor, lateral.reshape(1, cells), pairs, thermal)


def solution(mesh):
    in_specs = (P(None, "brick", None), P("grp", "brick", None), P(), P("brick"), P())
    out_specs = P(None, None, "brick")
    return jax.shard_map(local, mesh=mesh, in_specs=in_specs, out_specs=out_specs, check_vma=False)
```
